32 devices in a mesh: rve: 4 (over y, x), slab: 8 (over z, core).
Axes of the slice: x: 2, y: 2, z: 4, core: 2. Of those that a mesh axis runs over, the one named last changes fastest.
Arguments:
- displacement: float32 [32, 3, 128, 256], P('slab', None, 'rve'), parts along dimension 2, may hold values from -6 to 6
- load: float32 [32, 3, 128, 256], P('slab', None, 'rve'), parts along dimension 2, may hold values from -24 to 24
- phase: int32 [32, 128, 256], P('slab', 'rve'), parts along dimension 1, may hold values from 0 to 2
- moduli: float32 [2, 3], replicated, may hold values from 0.5 to 4
Outputs:
- solution: float32 [32, 3, 128, 256], P('slab', None, 'rve'), parts along dimension 2
- residual: float32 [32, 3, 128, 256], P('slab', None, 'rve'), parts along dimension 2
The draws below stay inside these ranges and needn't reach their ends.
There are 4 independent parts, one for each index of `rve`. The reference program is written for one: setup_inputs(seed, part) draws one part's arguments, and reference() takes and returns one part's arrays. A program takes and returns all parts, laid end to end along the dimension named above; an argument that names none is the same for every part. Nothing has to cross between parts.
All inputs are finite; a program needn't handle non-finite values.
Results may differ from the reference program's by a relative error of at most 0.00002.
Values sent between devices are 32-bit elements; how exact they have to be, the bound alone decides.
A program may use at most 64 MiB of HBM per device.

```python
import math
import jax
import jax.numpy as jnp

NX = 32
NY = 256
PHASES = 3
SWEEPS = 6
NZ = 32


def place_ends(result, key, least, largest):
    dims = result.shape
    index_at = [jax.random.randint(jax.random.fold_in(key, axis), (), 0, dims[axis]) for axis in range(len(dims))]
    result = result.at[tuple(index_at)].set(least)
    longest = dims.index(max(dims))
    index_at[longest] = (index_at[longest] + 1) % dims[longest]
    return result.at[tuple(index_at)].set(largest)


def level_of(key, extent, shards, least, largest):
    loudness, own = 1.0, jax.random.fold_in(key, 6)
    for axis_at, shards_of in shards:
        heights = jnp.exp(jax.random.uniform(jax.random.fold_in(own, axis_at), (shards_of,), jnp.float32, least / len(shards), largest / len(shards)))
        loudness = loudness * jnp.repeat(heights, extent[axis_at] // shards_of).reshape([-1 if axis == axis_at else 1 for axis in range(len(extent))])
    return loudness


def gaussian(own_key, shape, scale, reach, cuts=(), kind=jnp.bfloat16):
    result = scale * jax.random.normal(own_key, shape, jnp.float32)
    if cuts:
        result = result * level_of(own_key, shape, cuts, -0.22, 0.18)
    return jnp.clip(result, -reach, reach).astype(kind)


def setup_inputs(seed: int = 0, part: int = 0) -> dict:
    streams_of = jax.random.split(jax.random.key(seed), 5)
    part_keys = jax.random.split(jax.random.fold_in(streams_of[4], part), 5)
    return {
        "displacement": gaussian(part_keys[0], (NZ, 3, NX, NY), 1.0, 6.0, ((0, 8),), jnp.float32),
        "load": gaussian(part_keys[1], (NZ, 3, NX, NY), 4.0, 24.0, ((0, 8),), jnp.float32),
        "phase": place_ends(jax.random.randint(part_keys[2], (NZ, NX, NY), 0, PHASES), jax.random.fold_in(part_keys[2], 1), 0, PHASES - 1).astype(jnp.int32),
        "moduli": jnp.clip(jnp.exp(jax.random.uniform(streams_of[3], (2, PHASES), jnp.float32, math.log(0.5), math.log(4.0))), 0.5, 4.0),
    }


def plus_next(value, axis):
    return value + jnp.roll(value, -1, axis)


def minus_next(value, axis):
    return jnp.roll(value, -1, axis) - value


def plus_prev(value, axis):
    return value + jnp.roll(value, 1, axis)


def prev_minus(value, axis):
    return jnp.roll(value, 1, axis) - value


def materials(phase, moduli):
    lame = jnp.zeros(phase.shape, jnp.float32)
    shear = jnp.zeros(phase.shape, jnp.float32)
    for index in range(moduli.shape[1]):
        select = (phase == index).astype(jnp.float32)
        lame = lame + select * moduli[0, index]
        shear = shear + select * moduli[1, index]
    return lame, shear


def element_terms(lower, upper, lame, shear):
    total = lower + upper
    jump = upper - lower
    grad_x = 0.25 * minus_next(plus_next(total, -1), -2)
    grad_y = 0.25 * plus_next(minus_next(total, -1), -2)
    grad_z = 0.25 * plus_next(plus_next(jump, -1), -2)
    trace = grad_x[:, 0] + grad_y[:, 1] + grad_z[:, 2]
    normal_x = lame * trace + 2.0 * shear * grad_x[:, 0]
    normal_y = lame * trace + 2.0 * shear * grad_y[:, 1]
    normal_z = lame * trace + 2.0 * shear * grad_z[:, 2]
    shear_xy = shear * (grad_y[:, 0] + grad_x[:, 1])
    shear_xz = shear * (grad_z[:, 0] + grad_x[:, 2])
    shear_yz = shear * (grad_z[:, 1] + grad_y[:, 2])
    col_x = jnp.stack([normal_x, shear_xy, shear_xz], 1)
    col_y = jnp.stack([shear_xy, normal_y, shear_yz], 1)
    col_z = jnp.stack([shear_xz, shear_yz, normal_z], 1)
    inplane = 0.25 * (plus_prev(prev_minus(col_x, -2), -1) + plus_prev(prev_minus(col_y, -1), -2))
    vertical = 0.25 * plus_prev(plus_prev(col_z, -1), -2)
    return inplane, vertical


def operate(field, lame, shear):
    inplane, vertical = element_terms(field, jnp.roll(field, -1, 0), lame, shear)
    return inplane + jnp.roll(inplane, 1, 0) + jnp.roll(vertical, 1, 0) - vertical


def reference(displacement, load, phase, moduli):
    lame, shear = materials(phase, moduli)
    stiff = lame + 4.0 * shear
    diagonal = plus_prev(plus_prev(plus_prev(stiff, -1), -2), 0) / 16.0
    diagonal = diagonal[:, None]
    field = displacement
    for sweep in range(SWEEPS):
        field = field + 0.5 * (load - operate(field, lame, shear)) / diagonal
    return field, load - operate(field, lame, shear)
```

```python
import functools

import jax
import jax.numpy as jnp
from jax import lax
from jax.experimental import pallas as pl
from jax.experimental.pallas import tpu as pltpu
from jax.sharding import PartitionSpec as P

SWEEPS = 6
MESH = pl.DeviceIdType.MESH
ROWS = 8

STRESS = ((0, 3, 4), (3, 1, 5), (4, 5, 2))


def shift_next(value, axis):
    return pltpu.roll(value, value.shape[axis] - 1, axis)


def shift_prev(value, axis):
    return pltpu.roll(value, 1, axis)


def kernel(
    peers, disp, load, phase, moduli, out, rest,
    u, ld, ph, lam, mu, mu2, inv, fwd, st, res,
    in_sem, edge_send, edge_recv, send_sem, recv_sem, out_sem,
):
    local, _, nx, ny = disp.shape
    phases = moduli.shape[1]
    me = lax.axis_index("slab")
    above = lax.rem(me + 1, peers)
    below = lax.rem(me + peers - 1, peers)

    first = pltpu.make_async_copy(disp, u.at[0, pl.ds(2, local)], in_sem.at[0])
    second = pltpu.make_async_copy(phase, ph.at[pl.ds(2, local)], in_sem.at[1])
    third = pltpu.make_async_copy(load, ld.at[pl.ds(1, local)], in_sem.at[2])
    first.start()
    second.start()
    third.start()

    barrier = pltpu.get_barrier_semaphore()
    for peer in (below, above):
        pl.semaphore_signal(barrier, inc=1, device_id={"slab": peer}, device_id_type=MESH)
    pl.semaphore_wait(barrier, 2)

    edges = []

    def edge(src, dst, peer):
        at = len(edges)
        copy = pltpu.make_async_remote_copy(
            src_ref=src, dst_ref=dst, send_sem=edge_send.at[at], recv_sem=edge_recv.at[at],
            device_id={"slab": peer}, device_id_type=MESH,
        )
        copy.start()
        edges.append(copy)
        return copy

    first.wait()
    near_u = [edge(u.at[0, local + 1], u.at[0, 1], above), edge(u.at[0, 2], u.at[0, local + 2], below)]
    second.wait()
    near_ph = [edge(ph.at[local + 1], ph.at[1], above), edge(ph.at[2], ph.at[local + 2], below)]
    far_u = [edge(u.at[0, local], u.at[0, 0], above), edge(u.at[0, 3], u.at[0, local + 3], below)]
    far_ph = [edge(ph.at[local], ph.at[0], above)]
    third.wait()
    far_ld = [edge(ld.at[local], ld.at[0], above), edge(ld.at[1], ld.at[local + 1], below)]

    def sent(sweep, way):
        src, dst, peer = ((local, 0, above), (3, local + 3, below))[way]
        return pltpu.make_async_remote_copy(
            src_ref=u.at[sweep, src], dst_ref=u.at[sweep, dst],
            send_sem=send_sem.at[sweep, way], recv_sem=recv_sem.at[sweep, way],
            device_id={"slab": peer}, device_id_type=MESH,
        )

    def material(k):
        for r in range(0, nx, ROWS):
            at = pl.ds(r, ROWS)
            kind = ph[k + 2, at, :]
            lame = jnp.zeros(kind.shape, jnp.float32)
            shear = jnp.zeros(kind.shape, jnp.float32)
            for index in range(phases):
                lame = jnp.where(kind == index, moduli[0, index] * 0.0625, lame)
                shear = jnp.where(kind == index, moduli[1, index] * 0.0625, shear)
            lam[k + 2, at, :] = lame
            mu[k + 2, at, :] = shear
            mu2[k + 2, at, :] = shear + shear

    def diagonal(n):
        total = (lam[n + 1] + 2.0 * mu2[n + 1]) + (lam[n + 2] + 2.0 * mu2[n + 2])
        total = total + shift_prev(total, 1)
        total = total + shift_prev(total, 0)
        inv[n + 1] = 0.5 / total

    def forward(sweep, n):
        for c in range(3):
            value = u[sweep, n + 2, c]
            moved = shift_next(value, 1)
            total, jump = value + moved, moved - value
            moved = shift_next(total, 0)
            fwd[n + 2, c] = moved - total
            fwd[n + 2, 6 + c] = moved + total
            fwd[n + 2, 3 + c] = jump + shift_next(jump, 0)

    def element(k):
        lo, hi = k + 2, k + 3
        for r in range(0, nx, ROWS):
            at = pl.ds(r, ROWS)
            gx = [fwd[lo, c, at, :] + fwd[hi, c, at, :] for c in range(3)]
            gy = [fwd[lo, 3 + c, at, :] + fwd[hi, 3 + c, at, :] for c in range(3)]
            gz = [fwd[hi, 6 + c, at, :] - fwd[lo, 6 + c, at, :] for c in range(3)]
            bulk = lam[lo, at, :] * (gx[0] + gy[1] + gz[2])
            two, one = mu2[lo, at, :], mu[lo, at, :]
            st[lo, 0, at, :] = bulk + two * gx[0]
            st[lo, 1, at, :] = bulk + two * gy[1]
            st[lo, 2, at, :] = bulk + two * gz[2]
            st[lo, 3, at, :] = one * (gy[0] + gx[1])
            st[lo, 4, at, :] = one * (gz[0] + gx[2])
            st[lo, 5, at, :] = one * (gz[1] + gy[2])

    def remain(n, c):
        lo, hi = n + 1, n + 2
        x, y, z = STRESS[c]
        px = st[lo, x] + st[hi, x]
        rz = st[lo, z] - st[hi, z]
        qy = st[lo, y] + st[hi, y]
        e = (rz - px) + shift_prev(rz + px, 0)
        b = qy + shift_prev(qy, 0)
        return ld[n + 1, c] - ((e - b) + shift_prev(e + b, 1))

    def advance(sweep, n):
        for c in range(3):
            u[sweep, n + 2, c] = u[sweep - 1, n + 2, c] + inv[n + 1] * remain(n, c)

    def finish(n):
        for c in range(3):
            res[n, c] = remain(n, c)

    def inner(sweep):
        for n in range(local):
            forward(sweep - 1, n)
        for k in range(local - 1):
            element(k)

    def halo(sweep):
        forward(sweep - 1, -2)
        element(-2)
        advance(sweep, -1)
        forward(sweep - 1, local + 1)
        element(local)
        advance(sweep, local)

    def rim(sweep):
        forward(sweep, -1)
        element(-1)
        forward(sweep, local)
        element(local - 1)

    for k in range(local):
        material(k)
    for n in range(1, local):
        diagonal(n)
    inner(1)
    for n in range(1, local - 1):
        advance(1, n)
    for way in range(2):
        sent(1, way).start()
    for copy in near_u + near_ph:
        copy.wait_recv()
    material(-1)
    material(local)
    diagonal(0)
    diagonal(local)
    rim(0)
    advance(1, 0)
    advance(1, local - 1)

    def step(sweep, _):
        inner(sweep)
        for n in range(1, local - 1):
            advance(sweep, n)

        @pl.when(sweep < SWEEPS)
        def _():
            for way in range(2):
                sent(sweep, way).start()

        @pl.when(sweep == 2)
        def _():
            for copy in far_u + far_ph + far_ld:
                copy.wait_recv()
            material(-2)
            diagonal(-1)

        @pl.when(sweep > 2)
        def _():
            for way in range(2):
                sent(sweep - 2, way).wait_recv()

        halo(sweep - 1)
        rim(sweep - 1)
        advance(sweep, 0)
        advance(sweep, local - 1)
        return 0

    lax.fori_loop(2, SWEEPS + 1, step, 0)
    field_out = pltpu.make_async_copy(u.at[SWEEPS, pl.ds(2, local)], out, out_sem.at[0])
    field_out.start()

    inner(SWEEPS + 1)
    for n in range(1, local - 1):
        finish(n)
    for way in range(2):
        sent(SWEEPS - 1, way).wait_recv()
    halo(SWEEPS)
    rim(SWEEPS)
    finish(0)
    finish(local - 1)
    rest_out = pltpu.make_async_copy(res, rest, out_sem.at[1])
    rest_out.start()
    for copy in edges:
        copy.wait_send()
    for sweep in range(1, SWEEPS):
        for way in range(2):
            sent(sweep, way).wait_send()
    field_out.wait()
    rest_out.wait()


def on_device(peers, displacement, load, phase, moduli):
    local, comps, nx, ny = displacement.shape
    plane = (nx, ny)
    hbm = pl.BlockSpec(memory_space=pl.ANY)
    f32 = jnp.float32
    return pl.pallas_call(
        functools.partial(kernel, peers),
        out_shape=[jax.ShapeDtypeStruct(displacement.shape, f32)] * 2,
        in_specs=[hbm, hbm, hbm, pl.BlockSpec(memory_space=pltpu.SMEM)],
        out_specs=[hbm, hbm],
        scratch_shapes=[
            pltpu.VMEM((SWEEPS + 1, local + 4, comps) + plane, f32),
            pltpu.VMEM((local + 2, comps) + plane, f32),
            pltpu.VMEM((local + 3,) + plane, jnp.int32),
            pltpu.VMEM((local + 3,) + plane, f32),
            pltpu.VMEM((local + 3,) + plane, f32),
            pltpu.VMEM((local + 3,) + plane, f32),
            pltpu.VMEM((local + 2,) + plane, f32),
            pltpu.VMEM((local + 4, 9) + plane, f32),
            pltpu.VMEM((local + 3, 6) + plane, f32),
            pltpu.VMEM((local, comps) + plane, f32),
            pltpu.SemaphoreType.DMA((3,)),
            pltpu.SemaphoreType.DMA((9,)),
            pltpu.SemaphoreType.DMA((9,)),
            pltpu.SemaphoreType.DMA((SWEEPS + 1, 2)),
            pltpu.SemaphoreType.DMA((SWEEPS + 1, 2)),
            pltpu.SemaphoreType.DMA((2,)),
        ],
        compiler_params=pltpu.CompilerParams(collective_id=0, has_side_effects=True),
    )(displacement, load, phase, moduli)


def solution(mesh):
    in_specs = (
        P("slab", None, "rve", None),
        P("slab", None, "rve", None),
        P("slab", "rve", None),
        P(),
    )
    out_specs = (P("slab", None, "rve", None), P("slab", None, "rve", None))
    return jax.shard_map(
        functools.partial(on_device, mesh.shape["slab"]),
        mesh=mesh, in_specs=in_specs, out_specs=out_specs, check_vma=False,
    )
```

```python
import functools

import jax
import jax.numpy as jnp
from jax import lax
from jax.experimental import pallas as pl
from jax.experimental.pallas import tpu as pltpu
from jax.sharding import PartitionSpec as P

SWEEPS = 6
MESH = pl.DeviceIdType.MESH
ROWS = 8

STRESS = ((0, 3, 4), (3, 1, 5), (4, 5, 2))


def shift_next(value, axis):
    return pltpu.roll(value, value.shape[axis] - 1, axis)


def shift_prev(value, axis):
    return pltpu.roll(value, 1, axis)


def kernel(
    peers, disp, load, phase, moduli, out, rest,
    u, ld, ph, lam, mu, mu2, inv, fwd, st,
    in_sem, edge_send, edge_recv, send_sem, recv_sem,
):
    local, _, nx, ny = disp.shape
    phases = moduli.shape[1]
    me = lax.axis_index("slab")
    above = lax.rem(me + 1, peers)
    below = lax.rem(me + peers - 1, peers)

    first = pltpu.make_async_copy(disp, u.at[0, pl.ds(2, local)], in_sem.at[0])
    second = pltpu.make_async_copy(phase, ph.at[pl.ds(2, local)], in_sem.at[1])
    third = pltpu.make_async_copy(load, ld.at[pl.ds(1, local)], in_sem.at[2])
    first.start()
    second.start()
    third.start()

    barrier = pltpu.get_barrier_semaphore()
    for peer in (below, above):
        pl.semaphore_signal(barrier, inc=1, device_id={"slab": peer}, device_id_type=MESH)
    pl.semaphore_wait(barrier, 2)

    edges = []

    def edge(src, dst, peer):
        at = len(edges)
        copy = pltpu.make_async_remote_copy(
            src_ref=src, dst_ref=dst, send_sem=edge_send.at[at], recv_sem=edge_recv.at[at],
            device_id={"slab": peer}, device_id_type=MESH,
        )
        copy.start()
        edges.append(copy)
        return copy

    first.wait()
    near_u = [edge(u.at[0, local + 1], u.at[0, 1], above), edge(u.at[0, 2], u.at[0, local + 2], below)]
    second.wait()
    near_ph = [edge(ph.at[local + 1], ph.at[1], above), edge(ph.at[2], ph.at[local + 2], below)]
    far_u = [edge(u.at[0, local], u.at[0, 0], above), edge(u.at[0, 3], u.at[0, local + 3], below)]
    far_ph = [edge(ph.at[local], ph.at[0], above)]
    third.wait()
    far_ld = [edge(ld.at[local], ld.at[0], above), edge(ld.at[1], ld.at[local + 1], below)]

    def sent(sweep, way):
        src, dst, peer = ((local, 0, above), (3, local + 3, below))[way]
        return pltpu.make_async_remote_copy(
            src_ref=u.at[sweep, src], dst_ref=u.at[sweep, dst],
            send_sem=send_sem.at[sweep, way], recv_sem=recv_sem.at[sweep, way],
            device_id={"slab": peer}, device_id_type=MESH,
        )

    def material(k):
        for r in range(0, nx, ROWS):
            at = pl.ds(r, ROWS)
            kind = ph[k + 2, at, :]
            lame = jnp.zeros(kind.shape, jnp.float32)
            shear = jnp.zeros(kind.shape, jnp.float32)
            for index in range(phases):
                lame = jnp.where(kind == index, moduli[0, index] * 0.0625, lame)
                shear = jnp.where(kind == index, moduli[1, index] * 0.0625, shear)
            lam[k + 2, at, :] = lame
            mu[k + 2, at, :] = shear
            mu2[k + 2, at, :] = shear + shear

    def diagonal(n):
        total = (lam[n + 1] + 2.0 * mu2[n + 1]) + (lam[n + 2] + 2.0 * mu2[n + 2])
        total = total + shift_prev(total, 1)
        total = total + shift_prev(total, 0)
        inv[n + 1] = 0.5 / total

    def forward(sweep, n):
        for c in range(3):
            value = u[sweep, n + 2, c]
            moved = shift_next(value, 1)
            total, jump = value + moved, moved - value
            moved = shift_next(total, 0)
            fwd[n + 2, c] = moved - total
            fwd[n + 2, 6 + c] = moved + total
            fwd[n + 2, 3 + c] = jump + shift_next(jump, 0)

    def element(k):
        lo, hi = k + 2, k + 3
        for r in range(0, nx, ROWS):
            at = pl.ds(r, ROWS)
            gx = [fwd[lo, c, at, :] + fwd[hi, c, at, :] for c in range(3)]
            gy = [fwd[lo, 3 + c, at, :] + fwd[hi, 3 + c, at, :] for c in range(3)]
            gz = [fwd[hi, 6 + c, at, :] - fwd[lo, 6 + c, at, :] for c in range(3)]
            bulk = lam[lo, at, :] * (gx[0] + gy[1] + gz[2])
            two, one = mu2[lo, at, :], mu[lo, at, :]
            st[lo, 0, at, :] = bulk + two * gx[0]
            st[lo, 1, at, :] = bulk + two * gy[1]
            st[lo, 2, at, :] = bulk + two * gz[2]
            st[lo, 3, at, :] = one * (gy[0] + gx[1])
            st[lo, 4, at, :] = one * (gz[0] + gx[2])
            st[lo, 5, at, :] = one * (gz[1] + gy[2])

    def remain(n, c):
        lo, hi = n + 1, n + 2
        x, y, z = STRESS[c]
        px = st[lo, x] + st[hi, x]
        rz = st[lo, z] - st[hi, z]
        qy = st[lo, y] + st[hi, y]
        e = (rz - px) + shift_prev(rz + px, 0)
        b = qy + shift_prev(qy, 0)
        return ld[n + 1, c] - ((e - b) + shift_prev(e + b, 1))

    def advance(sweep, n):
        for c in range(3):
            u[sweep, n + 2, c] = u[sweep - 1, n + 2, c] + inv[n + 1] * remain(n, c)

    def finish(n):
        for c in range(3):
            rest[n, c] = remain(n, c)

    def inner(sweep):
        for n in range(local):
            forward(sweep - 1, n)
        for k in range(local - 1):
            element(k)

    def halo(sweep, side):
        forward(sweep - 1, (-2, local + 1)[side])
        element((-2, local)[side])
        advance(sweep, (-1, local)[side])

    def rim(sweep, side):
        forward(sweep, (-1, local)[side])
        element((-1, local - 1)[side])

    rims = (0, local - 1)

    for k in range(local):
        material(k)
    for n in range(1, local):
        diagonal(n)
    inner(1)
    for n in range(1, local - 1):
        advance(1, n)
    for way in range(2):
        sent(1, way).start()
    for side in range(2):
        near_u[side].wait_recv()
        near_ph[side].wait_recv()
        material((-1, local)[side])
        diagonal((0, local)[side])
        rim(0, side)
        advance(1, rims[side])

    def step(sweep, _):
        inner(sweep)
        for n in range(1, local - 1):
            advance(sweep, n)

        @pl.when(sweep < SWEEPS)
        def _():
            for way in range(2):
                sent(sweep, way).start()

        for side in range(2):

            @pl.when(sweep == 2)
            def _():
                far_u[side].wait_recv()
                far_ld[side].wait_recv()
                if side == 0:
                    far_ph[0].wait_recv()
                    material(-2)
                    diagonal(-1)

            @pl.when(sweep > 2)
            def _():
                sent(sweep - 2, side).wait_recv()

            halo(sweep - 1, side)
            rim(sweep - 1, side)
            advance(sweep, rims[side])
        return 0

    lax.fori_loop(2, SWEEPS + 1, step, 0)
    for n in range(1, local - 1):
        out[n] = u[SWEEPS, n + 2]
    out[0] = u[SWEEPS, 2]
    out[local - 1] = u[SWEEPS, local + 1]
    inner(SWEEPS + 1)
    for n in range(1, local - 1):
        finish(n)
    for side in range(2):
        sent(SWEEPS - 1, side).wait_recv()
        halo(SWEEPS, side)
        rim(SWEEPS, side)
        finish(rims[side])
    for copy in edges:
        copy.wait_send()
    for sweep in range(1, SWEEPS):
        for way in range(2):
            sent(sweep, way).wait_send()


def write_out(field, remain, out, rest, sem):
    copies = [pltpu.make_async_copy(field, out, sem.at[0]), pltpu.make_async_copy(remain, rest, sem.at[1])]
    for copy in copies:
        copy.start()
    for copy in copies:
        copy.wait()


def on_device(peers, displacement, load, phase, moduli):
    local, comps, nx, ny = displacement.shape
    plane = (nx, ny)
    hbm = pl.BlockSpec(memory_space=pl.ANY)
    f32 = jnp.float32
    vmem = pl.BlockSpec(memory_space=pltpu.VMEM)
    held = pl.pallas_call(
        functools.partial(kernel, peers),
        out_shape=[pltpu.VMEM(displacement.shape, f32)] * 2,
        in_specs=[hbm, hbm, hbm, pl.BlockSpec(memory_space=pltpu.SMEM)],
        out_specs=[vmem, vmem],
        scratch_shapes=[
            pltpu.VMEM((SWEEPS + 1, local + 4, comps) + plane, f32),
            pltpu.VMEM((local + 2, comps) + plane, f32),
            pltpu.VMEM((local + 3,) + plane, jnp.int32),
            pltpu.VMEM((local + 3,) + plane, f32),
            pltpu.VMEM((local + 3,) + plane, f32),
            pltpu.VMEM((local + 3,) + plane, f32),
            pltpu.VMEM((local + 2,) + plane, f32),
            pltpu.VMEM((local + 4, 9) + plane, f32),
            pltpu.VMEM((local + 3, 6) + plane, f32),
            pltpu.SemaphoreType.DMA((3,)),
            pltpu.SemaphoreType.DMA((9,)),
            pltpu.SemaphoreType.DMA((9,)),
            pltpu.SemaphoreType.DMA((SWEEPS + 1, 2)),
            pltpu.SemaphoreType.DMA((SWEEPS + 1, 2)),
        ],
        compiler_params=pltpu.CompilerParams(collective_id=0, has_side_effects=True),
    )(displacement, load, phase, moduli)
    return pl.pallas_call(
        write_out,
        out_shape=[jax.ShapeDtypeStruct(displacement.shape, f32)] * 2,
        in_specs=[hbm, hbm],
        out_specs=[hbm, hbm],
        scratch_shapes=[pltpu.SemaphoreType.DMA((2,))],
    )(*[pltpu.with_memory_space_constraint(one, pltpu.VMEM) for one in held])


def solution(mesh):
    in_specs = (
        P("slab", None, "rve", None),
        P("slab", None, "rve", None),
        P("slab", "rve", None),
        P(),
    )
    out_specs = (P("slab", None, "rve", None), P("slab", None, "rve", None))
    return jax.shard_map(
        functools.partial(on_device, mesh.shape["slab"]),
        mesh=mesh, in_specs=in_specs, out_specs=out_specs, check_vma=False,
    )
```

```python
import functools

import jax
import jax.numpy as jnp
from jax import lax
from jax.experimental import pallas as pl
from jax.experimental.pallas import tpu as pltpu
from jax.sharding import PartitionSpec as P

SWEEPS = 6
MESH = pl.DeviceIdType.MESH
ROWS = 8

STRESS = ((0, 3, 4), (3, 1, 5), (4, 5, 2))


def shift_next(value, axis):
    return pltpu.roll(value, value.shape[axis] - 1, axis)


def shift_prev(value, axis):
    return pltpu.roll(value, 1, axis)


def kernel(
    peers, disp, load, phase, moduli, out, rest,
    u, ld, ph, lam, mu, mu2, inv, fwd, st,
    in_sem, edge_send, edge_recv, send_sem, recv_sem,
):
    local, _, nx, ny = disp.shape
    phases = moduli.shape[1]
    me = lax.axis_index("slab")
    above = lax.rem(me + 1, peers)
    below = lax.rem(me + peers - 1, peers)

    first = pltpu.make_async_copy(disp, u.at[0, pl.ds(2, local)], in_sem.at[0])
    second = pltpu.make_async_copy(phase, ph.at[pl.ds(2, local)], in_sem.at[1])
    third = pltpu.make_async_copy(load, ld.at[pl.ds(1, local)], in_sem.at[2])
    first.start()
    second.start()
    third.start()

    barrier = pltpu.get_barrier_semaphore()
    for peer in (below, above):
        pl.semaphore_signal(barrier, inc=1, device_id={"slab": peer}, device_id_type=MESH)
    pl.semaphore_wait(barrier, 2)

    edges = []

    def edge(src, dst, peer):
        at = len(edges)
        copy = pltpu.make_async_remote_copy(
            src_ref=src, dst_ref=dst, send_sem=edge_send.at[at], recv_sem=edge_recv.at[at],
            device_id={"slab": peer}, device_id_type=MESH,
        )
        edges.append(copy)
        return copy

    near_u = [edge(u.at[0, local + 1], u.at[0, 1], above), edge(u.at[0, 2], u.at[0, local + 2], below)]
    near_ph = [edge(ph.at[local + 1], ph.at[1], above), edge(ph.at[2], ph.at[local + 2], below)]
    far_u = [edge(u.at[0, local], u.at[0, 0], above), edge(u.at[0, 3], u.at[0, local + 3], below)]
    far_ph = [edge(ph.at[local], ph.at[0], above)]
    far_ld = [edge(ld.at[local], ld.at[0], above), edge(ld.at[1], ld.at[local + 1], below)]
    closing = (me == peers - 1, me == 0)

    def far(way):
        far_u[way].start()
        if way == 0:
            far_ph[0].start()
        far_ld[way].start()

    first.wait()
    for copy in near_u:
        copy.start()
    second.wait()
    for copy in near_ph:
        copy.start()
    third.wait()
    for way in range(2):

        @pl.when(closing[way])
        def _():
            far(way)

    def sent(sweep, way):
        src, dst, peer = ((local, 0, above), (3, local + 3, below))[way]
        return pltpu.make_async_remote_copy(
            src_ref=u.at[sweep, src], dst_ref=u.at[sweep, dst],
            send_sem=send_sem.at[sweep, way], recv_sem=recv_sem.at[sweep, way],
            device_id={"slab": peer}, device_id_type=MESH,
        )

    def material(k):
        for r in range(0, nx, ROWS):
            at = pl.ds(r, ROWS)
            kind = ph[k + 2, at, :]
            lame = jnp.zeros(kind.shape, jnp.float32)
            shear = jnp.zeros(kind.shape, jnp.float32)
            for index in range(phases):
                lame = jnp.where(kind == index, moduli[0, index] * 0.0625, lame)
                shear = jnp.where(kind == index, moduli[1, index] * 0.0625, shear)
            lam[k + 2, at, :] = lame
            mu[k + 2, at, :] = shear
            mu2[k + 2, at, :] = shear + shear

    def diagonal(n):
        total = (lam[n + 1] + 2.0 * mu2[n + 1]) + (lam[n + 2] + 2.0 * mu2[n + 2])
        total = total + shift_prev(total, 1)
        total = total + shift_prev(total, 0)
        inv[n + 1] = 0.5 / total

    def forward(sweep, n):
        for c in range(3):
            value = u[sweep, n + 2, c]
            moved = shift_next(value, 1)
            total, jump = value + moved, moved - value
            moved = shift_next(total, 0)
            fwd[n + 2, c] = moved - total
            fwd[n + 2, 6 + c] = moved + total
            fwd[n + 2, 3 + c] = jump + shift_next(jump, 0)

    def element(k):
        lo, hi = k + 2, k + 3
        for r in range(0, nx, ROWS):
            at = pl.ds(r, ROWS)
            gx = [fwd[lo, c, at, :] + fwd[hi, c, at, :] for c in range(3)]
            gy = [fwd[lo, 3 + c, at, :] + fwd[hi, 3 + c, at, :] for c in range(3)]
            gz = [fwd[hi, 6 + c, at, :] - fwd[lo, 6 + c, at, :] for c in range(3)]
            bulk = lam[lo, at, :] * (gx[0] + gy[1] + gz[2])
            two, one = mu2[lo, at, :], mu[lo, at, :]
            st[lo, 0, at, :] = bulk + two * gx[0]
            st[lo, 1, at, :] = bulk + two * gy[1]
            st[lo, 2, at, :] = bulk + two * gz[2]
            st[lo, 3, at, :] = one * (gy[0] + gx[1])
            st[lo, 4, at, :] = one * (gz[0] + gx[2])
            st[lo, 5, at, :] = one * (gz[1] + gy[2])

    def remain(n, c):
        lo, hi = n + 1, n + 2
        x, y, z = STRESS[c]
        px = st[lo, x] + st[hi, x]
        rz = st[lo, z] - st[hi, z]
        qy = st[lo, y] + st[hi, y]
        e = (rz - px) + shift_prev(rz + px, 0)
        b = qy + shift_prev(qy, 0)
        return ld[n + 1, c] - ((e - b) + shift_prev(e + b, 1))

    def advance(sweep, n):
        for c in range(3):
            u[sweep, n + 2, c] = u[sweep - 1, n + 2, c] + inv[n + 1] * remain(n, c)

    def finish(n):
        for c in range(3):
            rest[n, c] = remain(n, c)

    rims = (0, local - 1)
    seconds = (1, local - 2)

    def middle(sweep):
        for n in range(1, local - 1):
            forward(sweep, n)
        for k in range(1, local - 2):
            element(k)

    def join(sweep, side):
        forward(sweep, rims[side])
        element((0, local - 2)[side])

    def halo(sweep, side):
        forward(sweep - 1, (-2, local + 1)[side])
        element((-2, local)[side])
        advance(sweep, (-1, local)[side])

    def rim(sweep, side):
        forward(sweep, (-1, local)[side])
        element((-1, local - 1)[side])

    for k in range(local):
        material(k)
    for n in range(1, local):
        diagonal(n)
    middle(0)
    for side in range(2):
        join(0, side)
    for n in range(1, local - 1):
        advance(1, n)
    for way in range(2):

        @pl.when(closing[way])
        def _():
            sent(1, way).start()

    middle(1)
    for n in range(2, local - 2):
        advance(2, n)
    for side in range(2):
        near_u[side].wait_recv()
        near_ph[side].wait_recv()
        material((-1, local)[side])
        diagonal((0, local)[side])
        if side == 0:
            for way in range(2):

                @pl.when(jnp.logical_not(closing[way]))
                def _():
                    far(way)
                    sent(1, way).start()

        rim(0, side)
        advance(1, rims[side])
        join(1, side)
        advance(2, seconds[side])
        sent(2, 1 - side).start()

    def step(sweep, _):
        middle(sweep)
        for n in range(2, local - 2):
            advance(sweep + 1, n)
        for side in range(2):

            @pl.when(sweep == 2)
            def _():
                far_u[side].wait_recv()
                far_ld[side].wait_recv()
                if side == 0:
                    far_ph[0].wait_recv()
                    material(-2)
                    diagonal(-1)

            @pl.when(sweep > 2)
            def _():
                sent(sweep - 2, side).wait_recv()

            halo(sweep - 1, side)
            rim(sweep - 1, side)
            advance(sweep, rims[side])
            join(sweep, side)
            advance(sweep + 1, seconds[side])

            @pl.when(sweep + 1 < SWEEPS)
            def _():
                sent(sweep + 1, 1 - side).start()

        return 0

    lax.fori_loop(2, SWEEPS, step, 0)

    middle(SWEEPS)
    for n in range(2, local - 2):
        finish(n)
    for n in range(1, local - 1):
        out[n] = u[SWEEPS, n + 2]
    for side in range(2):
        sent(SWEEPS - 2, side).wait_recv()
        halo(SWEEPS - 1, side)
        rim(SWEEPS - 1, side)
        advance(SWEEPS, rims[side])
        join(SWEEPS, side)
        finish(seconds[side])
    for n in rims:
        out[n] = u[SWEEPS, n + 2]
    for side in range(2):
        sent(SWEEPS - 1, side).wait_recv()
        halo(SWEEPS, side)
        rim(SWEEPS, side)
        finish(rims[side])
    for copy in edges:
        copy.wait_send()
    for sweep in range(1, SWEEPS):
        for way in range(2):
            sent(sweep, way).wait_send()


def write_out(field, remain, out, rest, sem):
    copies = [pltpu.make_async_copy(field, out, sem.at[0]), pltpu.make_async_copy(remain, rest, sem.at[1])]
    for copy in copies:
        copy.start()
    for copy in copies:
        copy.wait()


def on_device(peers, displacement, load, phase, moduli):
    local, comps, nx, ny = displacement.shape
    plane = (nx, ny)
    hbm = pl.BlockSpec(memory_space=pl.ANY)
    f32 = jnp.float32
    vmem = pl.BlockSpec(memory_space=pltpu.VMEM)
    held = pl.pallas_call(
        functools.partial(kernel, peers),
        out_shape=[pltpu.VMEM(displacement.shape, f32)] * 2,
        in_specs=[hbm, hbm, hbm, pl.BlockSpec(memory_space=pltpu.SMEM)],
        out_specs=[vmem, vmem],
        scratch_shapes=[
            pltpu.VMEM((SWEEPS + 1, local + 4, comps) + plane, f32),
            pltpu.VMEM((local + 2, comps) + plane, f32),
            pltpu.VMEM((local + 3,) + plane, jnp.int32),
            pltpu.VMEM((local + 3,) + plane, f32),
            pltpu.VMEM((local + 3,) + plane, f32),
            pltpu.VMEM((local + 3,) + plane, f32),
            pltpu.VMEM((local + 2,) + plane, f32),
            pltpu.VMEM((local + 4, 9) + plane, f32),
            pltpu.VMEM((local + 3, 6) + plane, f32),
            pltpu.SemaphoreType.DMA((3,)),
            pltpu.SemaphoreType.DMA((9,)),
            pltpu.SemaphoreType.DMA((9,)),
            pltpu.SemaphoreType.DMA((SWEEPS + 1, 2)),
            pltpu.SemaphoreType.DMA((SWEEPS + 1, 2)),
        ],
        compiler_params=pltpu.CompilerParams(collective_id=0, has_side_effects=True),
    )(displacement, load, phase, moduli)
    return pl.pallas_call(
        write_out,
        out_shape=[jax.ShapeDtypeStruct(displacement.shape, f32)] * 2,
        in_specs=[hbm, hbm],
        out_specs=[hbm, hbm],
        scratch_shapes=[pltpu.SemaphoreType.DMA((2,))],
    )(*[pltpu.with_memory_space_constraint(one, pltpu.VMEM) for one in held])


def solution(mesh):
    in_specs = (
        P("slab", None, "rve", None),
        P("slab", None, "rve", None),
        P("slab", "rve", None),
        P(),
    )
    out_specs = (P("slab", None, "rve", None), P("slab", None, "rve", None))
    return jax.shard_map(
        functools.partial(on_device, mesh.shape["slab"]),
        mesh=mesh, in_specs=in_specs, out_specs=out_specs, check_vma=False,
    )
```
